32 devices in a mesh: band: 8 (over z, x), gvec: 4 (over y, core).
Axes of the slice: x: 2, y: 2, z: 4, core: 2. Of those that a mesh axis runs over, the one named last changes fastest.
Arguments:
- wave_coeffs: bfloat16 [2, 256, 75264], P(None, 'band', 'gvec'), may hold values from -6 to 6
- projectors: bfloat16 [2, 64, 75264], P(None, 'band', 'gvec'), may hold values from -0.0234375 to 0.0234375
- miller_index: int32 [3, 75264], P(None, 'gvec'), may hold values from -24 to 24
- lattice: float32 [3, 3], replicated, may hold values from -0.25 to 1.25
- occupation: float32 [256], P('band'), may hold values from 0 to 2
- species: int32 [8], replicated, may hold values from 0 to 3
- proj_count: int32 [8], replicated, may hold values from 4 to 8
- coupling: float32 [4, 8, 8], replicated, may hold values from -0.4 to 2, as said below
Outputs:
- forces: float32 [3, 8], P(None, 'band')
- stress: float32 [3, 3], replicated
The draws below stay inside these ranges and needn't reach their ends.
Inputs may be any that keep to these rules, and one draw needn't show every extreme that they name: `coupling`: symmetric in its last two dimensions.
All inputs are finite; a program needn't handle non-finite values.
Results may differ from the reference program's by a relative error of at most 0.006.
Values may be sent and summed in bfloat16 or wider, within the bound.
A program may use at most 64 MiB of HBM per device.

```python
import math
import jax
import jax.numpy as jnp
from jax import lax

NG = 75264
PROJ = 8
NSPEC = 4
MILLER = 24
NATOMS = 8
NPROJ = 64
NBANDS = 256


def draw_lattice(key, part):
    spread = 0.15
    noise = jax.random.uniform(key, (3, 3), jnp.float32, -spread, spread)
    return jnp.eye(3, dtype=jnp.float32) + noise


def draw_occupation(key, part):
    center_key, width_key = jax.random.split(key)
    center = jax.random.uniform(center_key, (), jnp.float32, 0.4, 0.75) * NBANDS
    spread = jax.random.uniform(width_key, (), jnp.float32, 0.08, 0.15) * NBANDS
    position = jnp.arange(NBANDS, dtype=jnp.float32)
    return 2.0 / (1.0 + jnp.exp((position - center) / spread))


def draw_coupling(key, part):
    diag_key, off_key = jax.random.split(key)
    diagonal = jax.random.uniform(diag_key, (NSPEC, PROJ), jnp.float32, 0.5, 2.0)
    off_values = jax.random.uniform(off_key, (NSPEC, PROJ, PROJ), jnp.float32, -0.4, 0.4)
    symmetric = 0.5 * (off_values + jnp.swapaxes(off_values, 1, 2))
    identity = jnp.eye(PROJ, dtype=jnp.float32)
    return symmetric * (1.0 - identity) + diagonal[:, :, None] * identity


def set_ends(values, stream_key, low, largest):
    dims = values.shape
    place = [jax.random.randint(jax.random.fold_in(stream_key, axis), (), 0, dims[axis]) for axis in range(len(dims))]
    values = values.at[tuple(place)].set(low)
    longest = dims.index(max(dims))
    place[longest] = (place[longest] + 1) % dims[longest]
    return values.at[tuple(place)].set(largest)


def level_of(own_key, extent, cuts, low, high):
    factor_of, own = 1.0, jax.random.fold_in(own_key, 6)
    for axis_at, shards_of in cuts:
        draws = jnp.exp(jax.random.uniform(jax.random.fold_in(own, axis_at), (shards_of,), jnp.float32, low / len(cuts), high / len(cuts)))
        factor_of = factor_of * jnp.repeat(draws, extent[axis_at] // shards_of).reshape([-1 if axis == axis_at else 1 for axis in range(len(extent))])
    return factor_of


def bell_draw(own_key, dims, scale, bound, cuts=(), kind=jnp.bfloat16):
    values = scale * jax.random.normal(own_key, dims, jnp.float32)
    if cuts:
        values = values * level_of(own_key, dims, cuts, -0.22, 0.18)
    return jnp.clip(values, -bound, bound).astype(kind)


def setup_inputs(seed: int = 0) -> dict:
    keys = jax.random.split(jax.random.key(seed), 9)
    wave_coeffs = bell_draw(keys[0], (2, NBANDS, NG), 1.0, 6.0, ((1, 8), (2, 4)))
    projectors = bell_draw(keys[1], (2, NPROJ, NG), NG ** -0.5, 0.0234375, ((1, 8), (2, 4)))
    miller_index = set_ends(jax.random.randint(keys[2], (3, NG), -MILLER, MILLER + 1), jax.random.fold_in(keys[2], 1), -MILLER, MILLER).astype(jnp.int32)
    lattice = draw_lattice(jax.random.fold_in(keys[8], 71), 0)
    occupation = draw_occupation(jax.random.fold_in(keys[8], 71), 0)
    species = set_ends(jax.random.randint(keys[5], (NATOMS,), 0, NSPEC), jax.random.fold_in(keys[5], 1), 0, NSPEC - 1).astype(jnp.int32)
    proj_count = set_ends(jax.random.randint(keys[6], (NATOMS,), PROJ // 2, PROJ + 1), jax.random.fold_in(keys[6], 1), PROJ // 2, PROJ).astype(jnp.int32)
    coupling = draw_coupling(jax.random.fold_in(keys[8], 71), 0)
    return dict(wave_coeffs=wave_coeffs, projectors=projectors, miller_index=miller_index, lattice=lattice, occupation=occupation, species=species, proj_count=proj_count, coupling=coupling)


stress_pairs = ((0, 0), (1, 1), (2, 2), (0, 1), (0, 2), (1, 2))

def cart_weights(miller_index, lattice):
    indices = miller_index.astype(jnp.float32)
    coords = []
    for column in range(3):
        coords.append((indices[0] * lattice[0, column] + indices[1] * lattice[1, column] + indices[2] * lattice[2, column]) / MILLER)
    isotropic = (coords[0] * coords[0] + coords[1] * coords[1] + coords[2] * coords[2]) / 3.0
    weight_rows = [jnp.ones_like(coords[0])] + coords
    for first_axis, second_axis in stress_pairs:
        product = coords[first_axis] * coords[second_axis]
        if first_axis == second_axis:
            product = product - isotropic
        weight_rows.append(product)
    return jnp.stack(weight_rows)

def scale_block(weights, atom_block):
    proj_rows = atom_block.shape[1]
    scaled = (weights[:, None, None, :] * atom_block[None].astype(jnp.float32)).astype(jnp.bfloat16)
    return scaled.reshape(20 * proj_rows, atom_block.shape[2])

def intersection(scaled, flat_waves):
    product = lax.dot_general(scaled, flat_waves, (((1,), (1,)), ((), ())), preferred_element_type=jnp.float32)
    product = product.reshape(10, 2, scaled.shape[0] // 20, 2, flat_waves.shape[0] // 2)
    real_part = product[:, 0, :, 0] + product[:, 1, :, 1]
    imag_part = product[:, 0, :, 1] - product[:, 1, :, 0]
    return jnp.stack([real_part, imag_part], axis=1)

def atom_couplings(species, proj_count, coupling):
    kind_count = coupling.shape[0]
    proj_width = coupling.shape[1]
    onehot = (species[:, None] == jnp.arange(kind_count, dtype=jnp.int32)[None, :]).astype(jnp.float32)
    chosen = jnp.einsum('as,sij->aij', onehot, coupling, precision=lax.Precision.HIGHEST)
    active = (jnp.arange(proj_width, dtype=jnp.int32)[None, :] < proj_count[:, None]).astype(jnp.float32)
    return chosen * active[:, :, None] * active[:, None, :]

def contract(per_atom, couplings, occupied):
    mixed = jnp.einsum('aij,kcajn->kcain', couplings, per_atom, precision=lax.Precision.HIGHEST)
    becp_real = per_atom[0, 0]
    becp_imag = per_atom[0, 1]
    imag_sum = lax.optimization_barrier(jnp.sum(becp_real[None] * mixed[1:4, 1] - becp_imag[None] * mixed[1:4, 0], axis=2))
    real_sum = lax.optimization_barrier(jnp.sum(becp_real[None] * mixed[4:, 0] + becp_imag[None] * mixed[4:, 1], axis=2))
    force_part = lax.optimization_barrier(jnp.sum(imag_sum * occupied, axis=2))
    stress_part = lax.optimization_barrier(jnp.sum(real_sum * occupied, axis=(1, 2)))
    return (force_part, stress_part)

def stress_matrix(values):
    return jnp.stack([jnp.stack([values[0], values[3], values[4]]), jnp.stack([values[3], values[1], values[5]]), jnp.stack([values[4], values[5], values[2]])])

def reference(wave_coeffs, projectors, miller_index, lattice, occupation, species, proj_count, coupling):
    weights = cart_weights(miller_index, lattice)
    flat_waves = wave_coeffs.reshape(2 * NBANDS, NG)
    atom_blocks = projectors.reshape(2, NATOMS, PROJ, NG).transpose(1, 0, 2, 3)
    intersections = lax.map(lambda atom_block: intersection(scale_block(weights, atom_block), flat_waves), atom_blocks)
    per_atom = intersections.transpose(1, 2, 0, 3, 4)
    force_part, stress_part = contract(per_atom, atom_couplings(species, proj_count, coupling), occupation)
    force_scale = 2.0 / (PROJ * math.sqrt(NBANDS))
    stress_scale = 1.0 / (PROJ * math.sqrt(NATOMS * NBANDS))
    return (force_part * force_scale, stress_matrix(stress_part * stress_scale))
```

```python
import functools
import math

import jax
import jax.numpy as jnp
from jax import lax
from jax.experimental import pallas as pl
from jax.experimental.pallas import tpu as pltpu
from jax.sharding import PartitionSpec as P

PROJ = 8
MILLER = 24
LANES = 128
ALPHA = 0.45

stress_pairs = ((0, 0), (1, 1), (2, 2), (0, 1), (0, 2), (1, 2))


def largest_divisor(total, limit):
    return max(d for d in range(1, min(total, limit) + 1) if total % d == 0)


def piece_ranges(tiles):
    ring_tiles = int(round(ALPHA * tiles))
    cuts = [0, ring_tiles // 2, ring_tiles, ring_tiles + (tiles - ring_tiles) // 2, tiles]
    return [(cuts[i] * LANES, (cuts[i + 1] - cuts[i]) * LANES) for i in range(4)]


def swap_halves(values):
    half = values.shape[1] // 2
    return jnp.concatenate([values[:, half:], values[:, :half]], axis=1)


def kernel(
    bands, slots,
    waves_hbm, proj_hbm, miller_ref, lattice_ref, occupation_ref, species_ref, count_ref, coupling_ref,
    forces_ref, stress_ref,
    gath, waves, weights, spread, overlap, first_sum, second_sum,
    local_sem, send_sem, recv_sem, small_send, small_recv, first_send, first_recv, second_send, second_recv,
):
    me = lax.axis_index("band")
    slot = lax.axis_index("gvec")
    pair = 2 if bands % 2 == 0 else 1
    ring = bands // pair
    row = me // pair
    column = me % pair
    steps = ring // 2
    width = waves.shape[1]
    tiles = width // LANES
    wave_rows = waves.shape[0]
    ranges = piece_ranges(tiles)

    own_copy = pltpu.make_async_copy(proj_hbm, gath.at[me], local_sem.at[0])
    own_copy.start()
    wave_copy = pltpu.make_async_copy(waves_hbm, waves, local_sem.at[1])
    wave_copy.start()
    barrier = pltpu.get_barrier_semaphore()
    for offset in range(1, bands):
        pl.semaphore_signal(barrier, inc=1, device_id={"band": (me + offset) % bands}, device_id_type=pl.DeviceIdType.MESH)
    for offset in range(1, slots):
        pl.semaphore_signal(barrier, inc=1, device_id={"gvec": (slot + offset) % slots}, device_id_type=pl.DeviceIdType.MESH)
    own_copy.wait()
    pl.semaphore_wait(barrier, bands + slots - 2)

    sent = []

    def block_at(direction, step, other):
        at = (row - direction * step + ring * step) % ring
        return at * pair + ((column + 1) % pair if other else column)

    def piece_copy(block, piece, target, number):
        start, size = ranges[piece]
        part = gath.at[block, :, pl.ds(start, size)]
        return pltpu.make_async_remote_copy(
            src_ref=part, dst_ref=part, send_sem=send_sem.at[number], recv_sem=recv_sem.at[piece, block],
            device_id={"band": target}, device_id_type=pl.DeviceIdType.MESH,
        )

    def send(block, piece, target):
        if ranges[piece][1] == 0:
            return
        copy = piece_copy(block, piece, target, len(sent))
        copy.start()
        sent.append(copy)

    def arrive(block, piece):
        if ranges[piece][1]:
            piece_copy(block, piece, me, 0).wait_recv()

    def neighbour(direction):
        return ((row + direction + ring) % ring) * pair + column

    across = row * pair + (column + 1) % pair

    def pieces_of(direction, step, kind):
        if step > steps or step == 0:
            return []
        if ring % 2 == 0 and step == steps:
            return [kind * 2 + (0 if direction > 0 else 1)]
        return [kind * 2, kind * 2 + 1]

    directions = (1, -1)

    def forward_ring(block, direction, step, kind):
        for piece in pieces_of(direction, step + 1, kind):
            send(block, piece, neighbour(direction))

    if pair == 2:
        for piece in (2, 3):
            send(me, piece, across)
    for kind in (0, 1):
        for direction in directions:
            forward_ring(me, direction, 0, kind)
    if pair == 2:
        for piece in (0, 1):
            send(me, piece, across)

    weight_chunk = largest_divisor(tiles, 8) * LANES

    def weight_step(step, carry):
        at = pl.ds(pl.multiple_of(step * weight_chunk, LANES), weight_chunk)
        indices = miller_ref[:, at].astype(jnp.float32)
        coords = []
        for axis in range(3):
            total = (
                indices[0:1] * lattice_ref[0, axis]
                + indices[1:2] * lattice_ref[1, axis]
                + indices[2:3] * lattice_ref[2, axis]
            )
            coords.append(total * (1.0 / MILLER))
        isotropic = (coords[0] * coords[0] + coords[1] * coords[1] + coords[2] * coords[2]) * (1.0 / 3.0)
        for axis in range(3):
            weights[axis : axis + 1, at] = coords[axis]
        for index, (first_axis, second_axis) in enumerate(stress_pairs):
            product = coords[first_axis] * coords[second_axis]
            if first_axis == second_axis:
                product = product - isotropic
            weights[3 + index : 4 + index, at] = product
        spread[:, at] = jnp.zeros((PROJ, weight_chunk), jnp.float32)
        return carry

    lax.fori_loop(0, width // weight_chunk, weight_step, 0)
    wave_copy.wait()

    chunk = largest_divisor(tiles, 24) * LANES
    lane = lax.broadcasted_iota(jnp.int32, (8, LANES), 1)
    sublane = lax.broadcasted_iota(jnp.int32, (8, LANES), 0)
    half_lane = lax.broadcasted_iota(jnp.int32, (PROJ, wave_rows), 1) < wave_rows // 2
    sign = jnp.where(half_lane, 1.0, -1.0).astype(jnp.float32)
    occupied = jnp.concatenate([occupation_ref[...], occupation_ref[...]], axis=1)

    def small_copy(block, offset):
        part = overlap.at[block, slot]
        return pltpu.make_async_remote_copy(
            src_ref=part, dst_ref=part, send_sem=small_send.at[block, offset - 1],
            recv_sem=small_recv.at[block, offset - 1],
            device_id={"gvec": (slot + offset) % slots}, device_id_type=pl.DeviceIdType.MESH,
        )

    def small_arrival(block, offset):
        part = overlap.at[block, (slot + slots - offset) % slots]
        return pltpu.make_async_remote_copy(
            src_ref=part, dst_ref=part, send_sem=small_send.at[block, offset - 1],
            recv_sem=small_recv.at[block, offset - 1],
            device_id={"gvec": (slot + offset) % slots}, device_id_type=pl.DeviceIdType.MESH,
        )

    def project(block):
        def body(step, total):
            at = pl.ds(pl.multiple_of(step * chunk, LANES), chunk)
            return total + lax.dot_general(
                gath[block, :, at], waves[:, at], (((1,), (1,)), ((), ())), preferred_element_type=jnp.float32
            )

        product = lax.fori_loop(0, width // chunk, body, jnp.zeros((2 * PROJ, wave_rows), jnp.float32))
        becp = product[:PROJ] + sign * swap_halves(product[PROJ:])
        overlap[block, slot] = becp
        for offset in range(1, slots):
            small_copy(block, offset).start()

    def finish(block, part):
        for offset in range(1, slots):
            small_arrival(block, offset).wait_recv()
        becp = overlap[block, 0]
        for peer in range(1, slots):
            becp = becp + overlap[block, peer]
        matrix = jnp.zeros((PROJ, PROJ), jnp.float32)
        for kind in range(coupling_ref.shape[0]):
            matrix = matrix + jnp.where(species_ref[block] == kind, 1.0, 0.0) * coupling_ref[kind]
        active_row = lax.broadcasted_iota(jnp.int32, (PROJ, PROJ), 0) < count_ref[block]
        active_column = lax.broadcasted_iota(jnp.int32, (PROJ, PROJ), 1) < count_ref[block]
        matrix = jnp.where(active_row & active_column, matrix, 0.0)
        mixed = matrix[:, 0:1] * becp[0:1]
        for index in range(1, PROJ):
            mixed = mixed + matrix[:, index : index + 1] * becp[index : index + 1]
        mixed = mixed * occupied
        factors = jnp.concatenate([mixed, -sign * swap_halves(mixed)], axis=0)
        high = factors.astype(jnp.bfloat16)
        low = (factors - high.astype(jnp.float32)).astype(jnp.bfloat16)
        stacked = jnp.concatenate([high, low], axis=0)

        def body(step, sums):
            at = pl.ds(pl.multiple_of(step * chunk, LANES), chunk)
            both = jnp.dot(stacked, waves[:, at], preferred_element_type=jnp.float32)
            both = both[: 2 * PROJ] + both[2 * PROJ :]
            projectors = gath[block, :, at].astype(jnp.float32)
            proj_real, proj_imag = projectors[:PROJ], projectors[PROJ:]
            sum_real, sum_imag = both[:PROJ], both[PROJ:]
            imag_part = proj_real * sum_imag - proj_imag * sum_real
            spread[:, at] += proj_real * sum_real + proj_imag * sum_imag
            new = []
            for axis in range(3):
                weighted = imag_part * weights[axis : axis + 1, at]
                total = sums[axis]
                for tile in range(chunk // LANES):
                    total = total + weighted[:, tile * LANES : (tile + 1) * LANES]
                new.append(total)
            return tuple(new)

        zero = jnp.zeros((PROJ, LANES), jnp.float32)
        sums = lax.fori_loop(0, width // chunk, body, (zero, zero, zero))
        for axis in range(3):
            value = jnp.sum(jnp.sum(sums[axis], axis=0, keepdims=True), axis=1, keepdims=True)
            part = part + jnp.where((sublane == axis) & (lane == block), value, 0.0)
        return part

    state = {"part": jnp.zeros((8, LANES), jnp.float32), "waiting": None, "blocks": []}

    def work(block):
        project(block)
        state["blocks"].append(block)
        if state["waiting"] is not None:
            state["part"] = finish(state["waiting"], state["part"])
        state["waiting"] = block

    def ring_blocks(step, other):
        chosen = [block_at(1, step, other)]
        if not (ring % 2 == 0 and step == steps):
            chosen.append(block_at(-1, step, other))
        return chosen

    def take_ring(step, other, kind):
        for direction in directions:
            block = block_at(direction, step, other)
            for piece in pieces_of(direction, step, kind):
                arrive(block, piece)
                if piece in pieces_of(direction, step + 1, kind):
                    send(block, piece, neighbour(direction))
                if kind == 0 and not other and pair == 2:
                    send(block, piece, across)

    def take_across(step):
        for block in ring_blocks(step, True):
            for piece in (0, 1):
                arrive(block, piece)

    work(me)
    if pair == 2:
        for piece in (2, 3):
            arrive(across, piece)
            for direction in directions:
                if piece in pieces_of(direction, 1, 1):
                    send(across, piece, neighbour(direction))
        for piece in (0, 1):
            arrive(across, piece)
        work(across)
    for step in range(1, steps + 1):
        take_ring(step, False, 0)
        if step > 1 and pair == 2:
            take_across(step - 1)
            for block in ring_blocks(step - 1, True):
                work(block)
        take_ring(step, False, 1)
        if pair == 2:
            take_ring(step, True, 1)
        for block in ring_blocks(step, False):
            work(block)
    if pair == 2 and steps:
        take_across(steps)
        for block in ring_blocks(steps, True):
            work(block)
    part = finish(state["waiting"], state["part"])

    def stress_step(step, sums):
        at = pl.ds(pl.multiple_of(step * chunk, LANES), chunk)
        density = jnp.sum(spread[:, at], axis=0, keepdims=True)
        weighted = weights[:, at] * density
        for tile in range(chunk // LANES):
            sums = sums + weighted[:, tile * LANES : (tile + 1) * LANES]
        return sums

    weights[9:16, :] = jnp.zeros((7, width), jnp.float32)
    stress_sums = lax.fori_loop(0, width // chunk, stress_step, jnp.zeros((16, LANES), jnp.float32))
    stress_values = jnp.sum(stress_sums, axis=1, keepdims=True)[3:11]
    part = jnp.where(lane == LANES - 1, stress_values, part)

    def exchange(values, store, axis_name, index, count, send_sems, recv_sems):
        store[index] = values
        copies = []
        for offset in range(1, count):
            mine = store.at[index]
            copy = pltpu.make_async_remote_copy(
                src_ref=mine, dst_ref=mine, send_sem=send_sems.at[offset - 1], recv_sem=recv_sems.at[offset - 1],
                device_id={axis_name: (index + offset) % count}, device_id_type=pl.DeviceIdType.MESH,
            )
            copy.start()
            copies.append(copy)
        for offset in range(1, count):
            theirs = store.at[(index + count - offset) % count]
            pltpu.make_async_remote_copy(
                src_ref=theirs, dst_ref=theirs, send_sem=send_sems.at[offset - 1], recv_sem=recv_sems.at[offset - 1],
                device_id={axis_name: (index + offset) % count}, device_id_type=pl.DeviceIdType.MESH,
            ).wait_recv()
        total = store[0]
        for other in range(1, count):
            total = total + store[other]
        return total, copies

    total, first_copies = exchange(part, first_sum, "gvec", slot, slots, first_send, first_recv)
    total, second_copies = exchange(total, second_sum, "band", me, bands, second_send, second_recv)

    band_total = bands * (wave_rows // 2)
    force_scale = 2.0 / (PROJ * math.sqrt(band_total))
    stress_scale = 1.0 / (PROJ * math.sqrt(bands * band_total))
    own_force = jnp.sum(jnp.where(lane == me, total, 0.0), axis=1, keepdims=True)
    forces_ref[...] = own_force[:3] * force_scale
    line = lax.broadcasted_iota(jnp.int32, (3, 3), 0)
    place = lax.broadcasted_iota(jnp.int32, (3, 3), 1)
    matrix = jnp.zeros((3, 3), jnp.float32)
    for index, (first_axis, second_axis) in enumerate(stress_pairs):
        here = ((line == first_axis) & (place == second_axis)) | ((line == second_axis) & (place == first_axis))
        matrix = jnp.where(here, total[index : index + 1, LANES - 1 : LANES] * stress_scale, matrix)
    stress_ref[...] = matrix

    for copy in sent + first_copies + second_copies:
        copy.wait_send()
    for block in state["blocks"]:
        for offset in range(1, slots):
            small_copy(block, offset).wait_send()


def body(bands, slots, wave_coeffs, projectors, miller_index, lattice, occupation, species, proj_count, coupling):
    band_count, width = wave_coeffs.shape[1:]
    assert projectors.shape[1] == PROJ and width % LANES == 0 and bands < LANES
    vmem = pl.BlockSpec(memory_space=pltpu.VMEM)
    smem = pl.BlockSpec(memory_space=pltpu.SMEM)
    hbm = pl.BlockSpec(memory_space=pl.ANY)
    dma = pltpu.SemaphoreType.DMA
    sends = 12 * bands
    return pl.pallas_call(
        functools.partial(kernel, bands, slots),
        out_shape=(jax.ShapeDtypeStruct((3, 1), jnp.float32), jax.ShapeDtypeStruct((3, 3), jnp.float32)),
        in_specs=[hbm, hbm, vmem, smem, vmem, smem, smem, vmem],
        out_specs=(vmem, vmem),
        scratch_shapes=[
            pltpu.VMEM((bands, 2 * PROJ, width), jnp.bfloat16),
            pltpu.VMEM((2 * band_count, width), jnp.bfloat16),
            pltpu.VMEM((16, width), jnp.float32),
            pltpu.VMEM((PROJ, width), jnp.float32),
            pltpu.VMEM((bands, slots, PROJ, 2 * band_count), jnp.float32),
            pltpu.VMEM((slots, 8, LANES), jnp.float32),
            pltpu.VMEM((bands, 8, LANES), jnp.float32),
            dma((2,)),
            dma((sends,)),
            dma((4, bands)),
            dma((bands, slots - 1)),
            dma((bands, slots - 1)),
            dma((slots - 1,)),
            dma((slots - 1,)),
            dma((bands - 1,)),
            dma((bands - 1,)),
        ],
        compiler_params=pltpu.CompilerParams(collective_id=0, has_side_effects=True, vmem_limit_bytes=56 * 2**20),
    )(
        wave_coeffs.reshape(2 * band_count, width),
        projectors.reshape(2 * PROJ, width),
        miller_index,
        lattice,
        occupation.reshape(1, band_count),
        species,
        proj_count,
        coupling,
    )


def solution(mesh):
    return jax.shard_map(
        functools.partial(body, mesh.shape["band"], mesh.shape["gvec"]),
        mesh=mesh,
        in_specs=(
            P(None, "band", "gvec"),
            P(None, "band", "gvec"),
            P(None, "gvec"),
            P(),
            P("band"),
            P(),
            P(),
            P(),
        ),
        out_specs=(P(None, "band"), P()),
        check_vma=False,
    )
```

```python
import functools
import math

import jax
import jax.numpy as jnp
from jax import lax
from jax.experimental import pallas as pl
from jax.experimental.pallas import tpu as pltpu
from jax.sharding import PartitionSpec as P

PROJ = 8
MILLER = 24
LANES = 128
CHUNK_TILES = 40
PIECES = 2

stress_pairs = ((0, 0), (1, 1), (2, 2), (0, 1), (0, 2), (1, 2))
MESH = pl.DeviceIdType.MESH


def largest_divisor(total, limit):
    return max(d for d in range(1, min(total, limit) + 1) if total % d == 0)


def swap_halves(values, group):
    half = group // 2
    parts = []
    for start in range(0, values.shape[1], group):
        parts += [values[:, start + half : start + group], values[:, start : start + half]]
    return jnp.concatenate(parts, axis=1)


def kernel(
    bands, slots,
    waves_hbm, proj_hbm, miller_ref, lattice_ref, occupation_ref, species_ref, count_ref, coupling_ref,
    forces_ref, stress_ref,
    gath, waves, weights, spread, overlap, first_sum, second_sum, filling, part_ref,
    local_sem, send_sem, recv_sem, pair_send, pair_recv, small_send, small_recv,
    first_send, first_recv, second_send, second_recv,
):
    me = lax.axis_index("band")
    slot = lax.axis_index("gvec")
    pair = waves.shape[0]
    line = bands // pair
    row = me // pair
    column = me % pair
    other = (column + 1) % pair
    across = row * pair + other
    group = waves.shape[1]
    width = waves.shape[2]
    held_tiles = width // LANES
    skip = waves_hbm.shape[1] // LANES - held_tiles
    begin = pl.multiple_of(column * skip * LANES, LANES)
    other_begin = pl.multiple_of(other * skip * LANES, LANES)
    cuts = [held_tiles * i // PIECES * LANES for i in range(PIECES + 1)]
    peers = pair * slots
    rank = column * slots + slot

    def peer_id(index):
        return {"band": row * pair + index // slots, "gvec": index % slots}

    def line_id(position):
        return {"band": position * pair + column, "gvec": slot}

    own_copy = pltpu.make_async_copy(proj_hbm.at[:, pl.ds(begin, width)], gath.at[row, column], local_sem.at[0])
    own_copy.start()
    wave_copy = pltpu.make_async_copy(waves_hbm.at[:, pl.ds(begin, width)], waves.at[column], local_sem.at[1])
    wave_copy.start()
    barrier = pltpu.get_barrier_semaphore()
    for offset in range(1, peers):
        pl.semaphore_signal(barrier, inc=1, device_id=peer_id((rank + offset) % peers), device_id_type=MESH)
    for offset in range(1, line):
        pl.semaphore_signal(barrier, inc=1, device_id=line_id((row + offset) % line), device_id_type=MESH)
    lanes = occupation_ref[...]
    tiled = jnp.concatenate([lanes, lanes] * pair, axis=1)
    where_lane = lax.broadcasted_iota(jnp.int32, (8, pair * group), 1)
    filling[column] = jnp.where(where_lane // group == column, jnp.broadcast_to(tiled, where_lane.shape), 0.0)
    pl.semaphore_wait(barrier, peers + line - 2)

    pair_copies = []

    def pair_copy(source, target, number):
        return pltpu.make_async_remote_copy(
            src_ref=source, dst_ref=target, send_sem=pair_send.at[number], recv_sem=pair_recv.at[number],
            device_id={"band": across, "gvec": slot}, device_id_type=MESH,
        )

    if pair == 2:
        for piece in range(PIECES):
            start, size = cuts[piece], cuts[piece + 1] - cuts[piece]
            pair_copies.append(pair_copy(
                proj_hbm.at[:, pl.ds(pl.multiple_of(other_begin + start, LANES), size)],
                gath.at[row, column, :, pl.ds(start, size)], piece,
            ))
        pair_copies.append(pair_copy(filling.at[column], filling.at[column], PIECES))
        pair_copies.append(pair_copy(waves_hbm.at[:, pl.ds(other_begin, width)], waves.at[column], PIECES + 1))
        for copy in pair_copies:
            copy.start()

    def line_copy(position, source_column, piece, way, target):
        start, size = cuts[piece], cuts[piece + 1] - cuts[piece]
        part = gath.at[position, source_column, :, pl.ds(start, size)]
        return pltpu.make_async_remote_copy(
            src_ref=part, dst_ref=part, send_sem=send_sem.at[way, position, source_column, piece],
            recv_sem=recv_sem.at[position, source_column, piece],
            device_id=line_id(target), device_id_type=MESH,
        )

    def has_next(way):
        return row < line - 1 if way == 0 else row > 0

    def holds(way, step):
        return row >= step if way == 0 else row + step < line

    def origin(way, step):
        return row - step if way == 0 else row + step

    def following(way):
        return row + 1 if way == 0 else row - 1

    def pass_on(position, source_column, piece):
        for way in (0, 1):
            @pl.when(has_next(way))
            def _():
                line_copy(position, source_column, piece, way, following(way)).start()

    own_copy.wait()
    for piece in range(PIECES):
        pass_on(row, column, piece)

    weight_chunk = largest_divisor(held_tiles, 8) * LANES

    def weight_step(step, carry):
        at = pl.ds(pl.multiple_of(step * weight_chunk, LANES), weight_chunk)
        indices = miller_ref[:, pl.ds(pl.multiple_of(begin + step * weight_chunk, LANES), weight_chunk)].astype(jnp.float32)
        coords = []
        for axis in range(3):
            total = (
                indices[0:1] * lattice_ref[0, axis]
                + indices[1:2] * lattice_ref[1, axis]
                + indices[2:3] * lattice_ref[2, axis]
            )
            coords.append(total * (1.0 / MILLER))
        isotropic = (coords[0] * coords[0] + coords[1] * coords[1] + coords[2] * coords[2]) * (1.0 / 3.0)
        for axis in range(3):
            weights[axis : axis + 1, at] = coords[axis]
        for index, (first_axis, second_axis) in enumerate(stress_pairs):
            product = coords[first_axis] * coords[second_axis]
            if first_axis == second_axis:
                product = product - isotropic
            weights[3 + index : 4 + index, at] = product
        weights[9:16, at] = jnp.zeros((7, weight_chunk), jnp.float32)
        spread[:, at] = jnp.zeros((PROJ, weight_chunk), jnp.float32)
        return carry

    def make_weights():
        lax.fori_loop(0, width // weight_chunk, weight_step, 0)

    if pair == 2:
        for piece in range(PIECES):
            start, size = cuts[piece], cuts[piece + 1] - cuts[piece]
            part = gath.at[row, other, :, pl.ds(start, size)]
            pair_copy(part, part, piece).wait_recv()
            pass_on(row, other, piece)
    make_weights()
    part_ref[...] = jnp.zeros_like(part_ref)

    chunk = largest_divisor(held_tiles, CHUNK_TILES) * LANES
    rows = pair * PROJ
    lane = lax.broadcasted_iota(jnp.int32, (8, LANES), 1)
    sublane = lax.broadcasted_iota(jnp.int32, (8, LANES), 0)
    first_half = lax.broadcasted_iota(jnp.int32, (PROJ, pair * group), 1) % group < group // 2
    sign = jnp.where(first_half, 1.0, -1.0).astype(jnp.float32)

    def small_copy(position, offset, source, target):
        piece = overlap.at[position, source]
        return pltpu.make_async_remote_copy(
            src_ref=piece, dst_ref=piece, send_sem=small_send.at[position, offset - 1],
            recv_sem=small_recv.at[position, offset - 1], device_id=peer_id(target), device_id_type=MESH,
        )

    def outgoing(position, offset):
        return small_copy(position, offset, rank, (rank + offset) % peers)

    def incoming(position, offset):
        return small_copy(position, offset, (rank + peers - offset) % peers, (rank + offset) % peers)

    def block_rows(position, at):
        return jnp.concatenate([gath[position, index, :, at] for index in range(pair)], axis=0)

    def wave_chunk(at):
        return jnp.concatenate([waves[index, :, at] for index in range(pair)], axis=0)

    def project(position):
        def body(step, total):
            at = pl.ds(pl.multiple_of(step * chunk, LANES), chunk)
            return total + lax.dot_general(
                block_rows(position, at), wave_chunk(at), (((1,), (1,)), ((), ())), preferred_element_type=jnp.float32
            )

        product = lax.fori_loop(0, width // chunk, body, jnp.zeros((2 * rows, pair * group), jnp.float32))
        becp = []
        for index in range(pair):
            base = 2 * PROJ * index
            becp.append(product[base : base + PROJ] + sign * swap_halves(product[base + PROJ : base + 2 * PROJ], group))
        overlap[position, rank] = jnp.concatenate(becp, axis=0)
        for offset in range(1, peers):
            outgoing(position, offset).start()

    def atom_matrix(atom):
        matrix = jnp.zeros((PROJ, PROJ), jnp.float32)
        for kind in range(coupling_ref.shape[0]):
            matrix = matrix + jnp.where(species_ref[atom] == kind, 1.0, 0.0) * coupling_ref[kind]
        active_row = lax.broadcasted_iota(jnp.int32, (PROJ, PROJ), 0) < count_ref[atom]
        active_column = lax.broadcasted_iota(jnp.int32, (PROJ, PROJ), 1) < count_ref[atom]
        return jnp.where(active_row & active_column, matrix, 0.0)

    def finish(position):
        for offset in range(1, peers):
            incoming(position, offset).wait_recv()
        becp = overlap[position, 0]
        for peer in range(1, peers):
            becp = becp + overlap[position, peer]
        occupied = filling[0]
        for index in range(1, pair):
            occupied = occupied + filling[index]
        factors = []
        for index in range(pair):
            matrix = atom_matrix(position * pair + index)
            base = PROJ * index
            mixed = matrix[:, 0:1] * becp[base : base + 1]
            for term in range(1, PROJ):
                mixed = mixed + matrix[:, term : term + 1] * becp[base + term : base + term + 1]
            mixed = mixed * occupied
            factors += [mixed, -sign * swap_halves(mixed, group)]
        factors = jnp.concatenate(factors, axis=0)
        high = factors.astype(jnp.bfloat16)
        low = (factors - high.astype(jnp.float32)).astype(jnp.bfloat16)
        stacked = jnp.concatenate([high, low], axis=0)

        def body(step, sums):
            at = pl.ds(pl.multiple_of(step * chunk, LANES), chunk)
            both = jnp.dot(stacked, wave_chunk(at), preferred_element_type=jnp.float32)
            both = both[: 2 * rows] + both[2 * rows :]
            density = spread[:, at]
            new = []
            for index in range(pair):
                base = 2 * PROJ * index
                projectors = gath[position, index, :, at].astype(jnp.float32)
                proj_real, proj_imag = projectors[:PROJ], projectors[PROJ:]
                sum_real, sum_imag = both[base : base + PROJ], both[base + PROJ : base + 2 * PROJ]
                imag_part = proj_real * sum_imag - proj_imag * sum_real
                density = density + proj_real * sum_real + proj_imag * sum_imag
                for axis in range(3):
                    weighted = imag_part * weights[axis : axis + 1, at]
                    total = sums[index * 3 + axis]
                    for tile in range(chunk // LANES):
                        total = total + weighted[:, tile * LANES : (tile + 1) * LANES]
                    new.append(total)
            spread[:, at] = density
            return tuple(new)

        zero = jnp.zeros((PROJ, LANES), jnp.float32)
        sums = lax.fori_loop(0, width // chunk, body, (zero,) * (3 * pair))
        part = part_ref[...]
        for index in range(pair):
            for axis in range(3):
                value = jnp.sum(jnp.sum(sums[index * 3 + axis], axis=0, keepdims=True), axis=1, keepdims=True)
                part = part + jnp.where((sublane == axis) & (lane == position * pair + index), value, 0.0)
        part_ref[...] = part

    def take(step):
        for source in range(pair):
            for piece in range(PIECES):
                for way in (0, 1):
                    @pl.when(holds(way, step))
                    def _():
                        line_copy(origin(way, step), source, piece, way, row).wait_recv()

                        @pl.when(has_next(way))
                        def _():
                            line_copy(origin(way, step), source, piece, way, following(way)).start()

    def each(step, action):
        if step == 0:
            action(row)
            return
        for way in (0, 1):
            @pl.when(holds(way, step))
            def _():
                action(origin(way, step))

    for step in range(1, line - 1):
        take(step)
    wave_copy.wait()
    if pair == 2:
        pair_copy(filling.at[other], filling.at[other], PIECES).wait_recv()
        pair_copy(waves.at[other], waves.at[other], PIECES + 1).wait_recv()
        if held_tiles > skip:
            shared = pl.ds(0, (held_tiles - skip) * LANES)
            keep = jnp.where(column == 0, 1.0, 0.0).astype(jnp.bfloat16)
            for index in range(pair):
                waves[index, :, shared] = waves[index, :, shared] * keep
    for step in range(line):
        if step and step == line - 1:
            take(step)
        each(step, project)
        if step:
            each(step - 1, finish)
    each(line - 1, finish)

    def stress_step(step, sums):
        at = pl.ds(pl.multiple_of(step * chunk, LANES), chunk)
        density = jnp.sum(spread[:, at], axis=0, keepdims=True)
        weighted = weights[:, at] * density
        for tile in range(chunk // LANES):
            sums = sums + weighted[:, tile * LANES : (tile + 1) * LANES]
        return sums

    stress_sums = lax.fori_loop(0, width // chunk, stress_step, jnp.zeros((16, LANES), jnp.float32))
    stress_values = jnp.sum(stress_sums, axis=1, keepdims=True)[3:11]
    part = jnp.where(lane == LANES - 1, stress_values, part_ref[...])

    def exchange(values, store, target_of, index, count, send_sems, recv_sems):
        store[index] = values
        copies = []

        def part_copy(held, offset):
            return pltpu.make_async_remote_copy(
                src_ref=store.at[held], dst_ref=store.at[held], send_sem=send_sems.at[offset - 1],
                recv_sem=recv_sems.at[offset - 1], device_id=target_of((index + offset) % count), device_id_type=MESH,
            )

        for offset in range(1, count):
            copies.append(part_copy(index, offset))
            copies[-1].start()
        for offset in range(1, count):
            part_copy((index + count - offset) % count, offset).wait_recv()
        total = store[0]
        for held in range(1, count):
            total = total + store[held]
        return total, copies

    total, first_copies = exchange(part, first_sum, peer_id, rank, peers, first_send, first_recv)
    total, second_copies = exchange(total, second_sum, line_id, row, line, second_send, second_recv)

    band_total = bands * (group // 2)
    force_scale = 2.0 / (PROJ * math.sqrt(band_total))
    stress_scale = 1.0 / (PROJ * math.sqrt(bands * band_total))
    own_force = jnp.sum(jnp.where(lane == me, total, 0.0), axis=1, keepdims=True)
    forces_ref[...] = own_force[:3] * force_scale
    down = lax.broadcasted_iota(jnp.int32, (3, 3), 0)
    along = lax.broadcasted_iota(jnp.int32, (3, 3), 1)
    matrix = jnp.zeros((3, 3), jnp.float32)
    for index, (first_axis, second_axis) in enumerate(stress_pairs):
        here = ((down == first_axis) & (along == second_axis)) | ((down == second_axis) & (along == first_axis))
        matrix = jnp.where(here, total[index : index + 1, LANES - 1 : LANES] * stress_scale, matrix)
    stress_ref[...] = matrix

    for copy in pair_copies + first_copies + second_copies:
        copy.wait_send()
    for way in (0, 1):
        for step in range(line - 1):
            for source in range(pair):
                for piece in range(PIECES):
                    @pl.when(has_next(way) & holds(way, step))
                    def _():
                        line_copy(origin(way, step), source, piece, way, following(way)).wait_send()
    for position in range(line):
        for offset in range(1, peers):
            outgoing(position, offset).wait_send()


def body(bands, slots, wave_coeffs, projectors, miller_index, lattice, occupation, species, proj_count, coupling):
    band_count, width = wave_coeffs.shape[1:]
    assert projectors.shape[1] == PROJ and width % LANES == 0 and bands < LANES
    vmem = pl.BlockSpec(memory_space=pltpu.VMEM)
    smem = pl.BlockSpec(memory_space=pltpu.SMEM)
    hbm = pl.BlockSpec(memory_space=pl.ANY)
    dma = pltpu.SemaphoreType.DMA
    pair = 2 if bands % 2 == 0 else 1
    line = bands // pair
    peers = pair * slots
    held = -(-(width // LANES) // pair) * LANES
    return pl.pallas_call(
        functools.partial(kernel, bands, slots),
        out_shape=(jax.ShapeDtypeStruct((3, 1), jnp.float32), jax.ShapeDtypeStruct((3, 3), jnp.float32)),
        in_specs=[hbm, hbm, vmem, smem, vmem, smem, smem, vmem],
        out_specs=(vmem, vmem),
        scratch_shapes=[
            pltpu.VMEM((line, pair, 2 * PROJ, held), jnp.bfloat16),
            pltpu.VMEM((pair, 2 * band_count, held), jnp.bfloat16),
            pltpu.VMEM((16, held), jnp.float32),
            pltpu.VMEM((PROJ, held), jnp.float32),
            pltpu.VMEM((line, peers, pair * PROJ, pair * 2 * band_count), jnp.float32),
            pltpu.VMEM((peers, 8, LANES), jnp.float32),
            pltpu.VMEM((line, 8, LANES), jnp.float32),
            pltpu.VMEM((pair, 8, pair * 2 * band_count), jnp.float32),
            pltpu.VMEM((8, LANES), jnp.float32),
            dma((2,)),
            dma((2, line, pair, PIECES)),
            dma((line, pair, PIECES)),
            dma((PIECES + 2,)),
            dma((PIECES + 2,)),
            dma((line, peers - 1)),
            dma((line, peers - 1)),
            dma((peers - 1,)),
            dma((peers - 1,)),
            dma((line - 1,)),
            dma((line - 1,)),
        ],
        compiler_params=pltpu.CompilerParams(collective_id=0, has_side_effects=True, vmem_limit_bytes=56 * 2**20),
    )(
        wave_coeffs.reshape(2 * band_count, width),
        projectors.reshape(2 * PROJ, width),
        miller_index,
        lattice,
        occupation.reshape(1, band_count),
        species,
        proj_count,
        coupling,
    )


def solution(mesh):
    return jax.shard_map(
        functools.partial(body, mesh.shape["band"], mesh.shape["gvec"]),
        mesh=mesh,
        in_specs=(
            P(None, "band", "gvec"),
            P(None, "band", "gvec"),
            P(None, "gvec"),
            P(),
            P("band"),
            P(),
            P(),
            P(),
        ),
        out_specs=(P(None, "band"), P()),
        check_vma=False,
    )
```

```python
import functools
import math

import jax
import jax.numpy as jnp
from jax import lax
from jax.experimental import pallas as pl
from jax.experimental.pallas import tpu as pltpu
from jax.sharding import PartitionSpec as P

PROJ = 8
MILLER = 24
LANES = 128
CHUNK_TILES = 40
PIECES = 2

stress_pairs = ((0, 0), (1, 1), (2, 2), (0, 1), (0, 2), (1, 2))
MESH = pl.DeviceIdType.MESH


def largest_divisor(total, limit):
    return max(d for d in range(1, min(total, limit) + 1) if total % d == 0)


def swap_halves(values, group):
    half = group // 2
    parts = []
    for start in range(0, values.shape[1], group):
        parts += [values[:, start + half : start + group], values[:, start : start + half]]
    return jnp.concatenate(parts, axis=1)


def kernel(
    bands, slots,
    waves_hbm, proj_hbm, miller_hbm, lattice_ref, occupation_ref, species_ref, count_ref, coupling_ref,
    forces_ref, stress_ref,
    gath, waves, weights, spread, overlap, first_sum, second_sum, filling, part_ref, miller_ref,
    local_sem, send_sem, recv_sem, pair_send, pair_recv, small_send, small_recv,
    first_send, first_recv, second_send, second_recv,
):
    me = lax.axis_index("band")
    slot = lax.axis_index("gvec")
    pair = waves.shape[0]
    line = bands // pair
    row = me // pair
    column = me % pair
    other = (column + 1) % pair
    across = row * pair + other
    group = waves.shape[1]
    width = waves.shape[2]
    held_tiles = width // LANES
    skip = waves_hbm.shape[1] // LANES - held_tiles
    begin = pl.multiple_of(column * skip * LANES, LANES)
    other_begin = pl.multiple_of(other * skip * LANES, LANES)
    cuts = [held_tiles * i // PIECES * LANES for i in range(PIECES + 1)]
    peers = pair * slots
    rank = column * slots + slot

    def peer_id(index):
        return {"band": row * pair + index // slots, "gvec": index % slots}

    def line_id(position):
        return {"band": position * pair + column, "gvec": slot}

    own_copy = pltpu.make_async_copy(proj_hbm.at[:, pl.ds(begin, width)], gath.at[row, column], local_sem.at[0])
    own_copy.start()
    wave_copy = pltpu.make_async_copy(waves_hbm.at[:, pl.ds(begin, width)], waves.at[column], local_sem.at[1])
    wave_copy.start()
    miller_copy = pltpu.make_async_copy(miller_hbm, miller_ref, local_sem.at[2])
    miller_copy.start()
    barrier = pltpu.get_barrier_semaphore()
    for offset in range(1, peers):
        pl.semaphore_signal(barrier, inc=1, device_id=peer_id((rank + offset) % peers), device_id_type=MESH)
    for offset in range(1, line):
        pl.semaphore_signal(barrier, inc=1, device_id=line_id((row + offset) % line), device_id_type=MESH)
    lanes = occupation_ref[...]
    tiled = jnp.concatenate([lanes, lanes] * pair, axis=1)
    where_lane = lax.broadcasted_iota(jnp.int32, (8, pair * group), 1)
    filling[column] = jnp.where(where_lane // group == column, jnp.broadcast_to(tiled, where_lane.shape), 0.0)
    pl.semaphore_wait(barrier, peers + line - 2)

    pair_copies = []

    def pair_copy(source, target, number):
        return pltpu.make_async_remote_copy(
            src_ref=source, dst_ref=target, send_sem=pair_send.at[number], recv_sem=pair_recv.at[number],
            device_id={"band": across, "gvec": slot}, device_id_type=MESH,
        )

    if pair == 2:
        for piece in range(PIECES):
            start, size = cuts[piece], cuts[piece + 1] - cuts[piece]
            pair_copies.append(pair_copy(
                proj_hbm.at[:, pl.ds(pl.multiple_of(other_begin + start, LANES), size)],
                gath.at[row, column, :, pl.ds(start, size)], piece,
            ))
        pair_copies.append(pair_copy(filling.at[column], filling.at[column], PIECES))
        pair_copies.append(pair_copy(waves_hbm.at[:, pl.ds(other_begin, width)], waves.at[column], PIECES + 1))
        for copy in pair_copies:
            copy.start()

    def line_copy(position, source_column, piece, way, target):
        start, size = cuts[piece], cuts[piece + 1] - cuts[piece]
        part = gath.at[position, source_column, :, pl.ds(start, size)]
        return pltpu.make_async_remote_copy(
            src_ref=part, dst_ref=part, send_sem=send_sem.at[way, position, source_column, piece],
            recv_sem=recv_sem.at[position, source_column, piece],
            device_id=line_id(target), device_id_type=MESH,
        )

    def has_next(way):
        return row < line - 1 if way == 0 else row > 0

    def holds(way, step):
        return row >= step if way == 0 else row + step < line

    def origin(way, step):
        return row - step if way == 0 else row + step

    def following(way):
        return row + 1 if way == 0 else row - 1

    def pass_on(position, source_column, piece):
        for way in (0, 1):
            @pl.when(has_next(way))
            def _():
                line_copy(position, source_column, piece, way, following(way)).start()

    own_copy.wait()
    for piece in range(PIECES):
        pass_on(row, column, piece)

    weight_chunk = largest_divisor(held_tiles, 8) * LANES

    def weight_step(step, carry):
        at = pl.ds(pl.multiple_of(step * weight_chunk, LANES), weight_chunk)
        indices = miller_ref[:, pl.ds(pl.multiple_of(begin + step * weight_chunk, LANES), weight_chunk)].astype(jnp.float32)
        coords = []
        for axis in range(3):
            total = (
                indices[0:1] * lattice_ref[0, axis]
                + indices[1:2] * lattice_ref[1, axis]
                + indices[2:3] * lattice_ref[2, axis]
            )
            coords.append(total * (1.0 / MILLER))
        isotropic = (coords[0] * coords[0] + coords[1] * coords[1] + coords[2] * coords[2]) * (1.0 / 3.0)
        for axis in range(3):
            weights[axis : axis + 1, at] = coords[axis]
        for index, (first_axis, second_axis) in enumerate(stress_pairs):
            product = coords[first_axis] * coords[second_axis]
            if first_axis == second_axis:
                product = product - isotropic
            weights[3 + index : 4 + index, at] = product
        weights[9:16, at] = jnp.zeros((7, weight_chunk), jnp.float32)
        spread[:, at] = jnp.zeros((PROJ, weight_chunk), jnp.float32)
        return carry

    def make_weights():
        lax.fori_loop(0, width // weight_chunk, weight_step, 0)

    if pair == 2:
        for piece in range(PIECES):
            start, size = cuts[piece], cuts[piece + 1] - cuts[piece]
            part = gath.at[row, other, :, pl.ds(start, size)]
            pair_copy(part, part, piece).wait_recv()
            pass_on(row, other, piece)
    miller_copy.wait()
    make_weights()
    part_ref[...] = jnp.zeros_like(part_ref)

    chunk = largest_divisor(held_tiles, CHUNK_TILES) * LANES
    rows = pair * PROJ
    lane = lax.broadcasted_iota(jnp.int32, (8, LANES), 1)
    sublane = lax.broadcasted_iota(jnp.int32, (8, LANES), 0)
    first_half = lax.broadcasted_iota(jnp.int32, (PROJ, pair * group), 1) % group < group // 2
    sign = jnp.where(first_half, 1.0, -1.0).astype(jnp.float32)

    def small_copy(position, offset, source, target):
        piece = overlap.at[position, source]
        return pltpu.make_async_remote_copy(
            src_ref=piece, dst_ref=piece, send_sem=small_send.at[position, offset - 1],
            recv_sem=small_recv.at[position, offset - 1], device_id=peer_id(target), device_id_type=MESH,
        )

    def outgoing(position, offset):
        return small_copy(position, offset, rank, (rank + offset) % peers)

    def incoming(position, offset):
        return small_copy(position, offset, (rank + peers - offset) % peers, (rank + offset) % peers)

    def block_rows(position, at):
        return jnp.concatenate([gath[position, index, :, at] for index in range(pair)], axis=0)

    def wave_chunk(at):
        return jnp.concatenate([waves[index, :, at] for index in range(pair)], axis=0)

    def project(position):
        def body(step, total):
            at = pl.ds(pl.multiple_of(step * chunk, LANES), chunk)
            return total + lax.dot_general(
                block_rows(position, at), wave_chunk(at), (((1,), (1,)), ((), ())), preferred_element_type=jnp.float32
            )

        product = lax.fori_loop(0, width // chunk, body, jnp.zeros((2 * rows, pair * group), jnp.float32))
        becp = []
        for index in range(pair):
            base = 2 * PROJ * index
            becp.append(product[base : base + PROJ] + sign * swap_halves(product[base + PROJ : base + 2 * PROJ], group))
        overlap[position, rank] = jnp.concatenate(becp, axis=0)
        for offset in range(1, peers):
            outgoing(position, offset).start()

    def atom_matrix(atom):
        matrix = jnp.zeros((PROJ, PROJ), jnp.float32)
        for kind in range(coupling_ref.shape[0]):
            matrix = matrix + jnp.where(species_ref[atom] == kind, 1.0, 0.0) * coupling_ref[kind]
        active_row = lax.broadcasted_iota(jnp.int32, (PROJ, PROJ), 0) < count_ref[atom]
        active_column = lax.broadcasted_iota(jnp.int32, (PROJ, PROJ), 1) < count_ref[atom]
        return jnp.where(active_row & active_column, matrix, 0.0)

    def finish(position):
        for offset in range(1, peers):
            incoming(position, offset).wait_recv()
        becp = overlap[position, 0]
        for peer in range(1, peers):
            becp = becp + overlap[position, peer]
        occupied = filling[0]
        for index in range(1, pair):
            occupied = occupied + filling[index]
        factors = []
        for index in range(pair):
            matrix = atom_matrix(position * pair + index)
            base = PROJ * index
            mixed = matrix[:, 0:1] * becp[base : base + 1]
            for term in range(1, PROJ):
                mixed = mixed + matrix[:, term : term + 1] * becp[base + term : base + term + 1]
            mixed = mixed * occupied
            factors += [mixed, -sign * swap_halves(mixed, group)]
        factors = jnp.concatenate(factors, axis=0)
        high = factors.astype(jnp.bfloat16)
        low = (factors - high.astype(jnp.float32)).astype(jnp.bfloat16)
        stacked = jnp.concatenate([high, low], axis=0)

        def body(step, sums):
            at = pl.ds(pl.multiple_of(step * chunk, LANES), chunk)
            both = jnp.dot(stacked, wave_chunk(at), preferred_element_type=jnp.float32)
            both = both[: 2 * rows] + both[2 * rows :]
            density = spread[:, at]
            new = []
            for index in range(pair):
                base = 2 * PROJ * index
                projectors = gath[position, index, :, at].astype(jnp.float32)
                proj_real, proj_imag = projectors[:PROJ], projectors[PROJ:]
                sum_real, sum_imag = both[base : base + PROJ], both[base + PROJ : base + 2 * PROJ]
                imag_part = proj_real * sum_imag - proj_imag * sum_real
                density = density + proj_real * sum_real + proj_imag * sum_imag
                for axis in range(3):
                    weighted = imag_part * weights[axis : axis + 1, at]
                    total = sums[index * 3 + axis]
                    for tile in range(chunk // LANES):
                        total = total + weighted[:, tile * LANES : (tile + 1) * LANES]
                    new.append(total)
            spread[:, at] = density
            return tuple(new)

        zero = jnp.zeros((PROJ, LANES), jnp.float32)
        sums = lax.fori_loop(0, width // chunk, body, (zero,) * (3 * pair))
        part = part_ref[...]
        for index in range(pair):
            for axis in range(3):
                value = jnp.sum(jnp.sum(sums[index * 3 + axis], axis=0, keepdims=True), axis=1, keepdims=True)
                part = part + jnp.where((sublane == axis) & (lane == position * pair + index), value, 0.0)
        part_ref[...] = part

    def take(step):
        for source in range(pair):
            for piece in range(PIECES):
                for way in (0, 1):
                    @pl.when(holds(way, step))
                    def _():
                        line_copy(origin(way, step), source, piece, way, row).wait_recv()

                        @pl.when(has_next(way))
                        def _():
                            line_copy(origin(way, step), source, piece, way, following(way)).start()

    def each(step, action):
        if step == 0:
            action(row)
            return
        for way in (0, 1):
            @pl.when(holds(way, step))
            def _():
                action(origin(way, step))

    for step in range(1, line - 1):
        take(step)
    wave_copy.wait()
    if pair == 2:
        pair_copy(filling.at[other], filling.at[other], PIECES).wait_recv()
        pair_copy(waves.at[other], waves.at[other], PIECES + 1).wait_recv()
        if held_tiles > skip:
            shared = pl.ds(0, (held_tiles - skip) * LANES)
            keep = jnp.where(column == 0, 1.0, 0.0).astype(jnp.bfloat16)
            for index in range(pair):
                waves[index, :, shared] = waves[index, :, shared] * keep
    for step in range(line):
        last = step > 0 and step == line - 1
        if last:
            each(step - 1, finish)
            take(step)
        each(step, project)
        if step and not last:
            each(step - 1, finish)
    each(line - 1, finish)

    def stress_step(step, sums):
        at = pl.ds(pl.multiple_of(step * chunk, LANES), chunk)
        density = jnp.sum(spread[:, at], axis=0, keepdims=True)
        weighted = weights[:, at] * density
        for tile in range(chunk // LANES):
            sums = sums + weighted[:, tile * LANES : (tile + 1) * LANES]
        return sums

    stress_sums = lax.fori_loop(0, width // chunk, stress_step, jnp.zeros((16, LANES), jnp.float32))
    stress_values = jnp.sum(stress_sums, axis=1, keepdims=True)[3:11]
    part = jnp.where(lane == LANES - 1, stress_values, part_ref[...])

    def exchange(values, store, target_of, index, count, send_sems, recv_sems):
        store[index] = values
        copies = []

        def part_copy(held, offset):
            return pltpu.make_async_remote_copy(
                src_ref=store.at[held], dst_ref=store.at[held], send_sem=send_sems.at[offset - 1],
                recv_sem=recv_sems.at[offset - 1], device_id=target_of((index + offset) % count), device_id_type=MESH,
            )

        for offset in range(1, count):
            copies.append(part_copy(index, offset))
            copies[-1].start()
        for offset in range(1, count):
            part_copy((index + count - offset) % count, offset).wait_recv()
        total = store[0]
        for held in range(1, count):
            total = total + store[held]
        return total, copies

    total, first_copies = exchange(part, first_sum, peer_id, rank, peers, first_send, first_recv)
    total, second_copies = exchange(total, second_sum, line_id, row, line, second_send, second_recv)

    band_total = bands * (group // 2)
    force_scale = 2.0 / (PROJ * math.sqrt(band_total))
    stress_scale = 1.0 / (PROJ * math.sqrt(bands * band_total))
    own_force = jnp.sum(jnp.where(lane == me, total, 0.0), axis=1, keepdims=True)
    forces_ref[...] = own_force[:3] * force_scale
    down = lax.broadcasted_iota(jnp.int32, (3, 3), 0)
    along = lax.broadcasted_iota(jnp.int32, (3, 3), 1)
    matrix = jnp.zeros((3, 3), jnp.float32)
    for index, (first_axis, second_axis) in enumerate(stress_pairs):
        here = ((down == first_axis) & (along == second_axis)) | ((down == second_axis) & (along == first_axis))
        matrix = jnp.where(here, total[index : index + 1, LANES - 1 : LANES] * stress_scale, matrix)
    stress_ref[...] = matrix

    for copy in pair_copies + first_copies + second_copies:
        copy.wait_send()
    for way in (0, 1):
        for step in range(line - 1):
            for source in range(pair):
                for piece in range(PIECES):
                    @pl.when(has_next(way) & holds(way, step))
                    def _():
                        line_copy(origin(way, step), source, piece, way, following(way)).wait_send()
    for position in range(line):
        for offset in range(1, peers):
            outgoing(position, offset).wait_send()


def body(bands, slots, wave_coeffs, projectors, miller_index, lattice, occupation, species, proj_count, coupling):
    band_count, width = wave_coeffs.shape[1:]
    assert projectors.shape[1] == PROJ and width % LANES == 0 and bands < LANES
    vmem = pl.BlockSpec(memory_space=pltpu.VMEM)
    smem = pl.BlockSpec(memory_space=pltpu.SMEM)
    hbm = pl.BlockSpec(memory_space=pl.ANY)
    dma = pltpu.SemaphoreType.DMA
    pair = 2 if bands % 2 == 0 else 1
    line = bands // pair
    peers = pair * slots
    held = -(-(width // LANES) // pair) * LANES
    return pl.pallas_call(
        functools.partial(kernel, bands, slots),
        out_shape=(jax.ShapeDtypeStruct((3, 1), jnp.float32), jax.ShapeDtypeStruct((3, 3), jnp.float32)),
        in_specs=[hbm, hbm, hbm, smem, vmem, smem, smem, vmem],
        out_specs=(vmem, vmem),
        scratch_shapes=[
            pltpu.VMEM((line, pair, 2 * PROJ, held), jnp.bfloat16),
            pltpu.VMEM((pair, 2 * band_count, held), jnp.bfloat16),
            pltpu.VMEM((16, held), jnp.float32),
            pltpu.VMEM((PROJ, held), jnp.float32),
            pltpu.VMEM((line, peers, pair * PROJ, pair * 2 * band_count), jnp.float32),
            pltpu.VMEM((peers, 8, LANES), jnp.float32),
            pltpu.VMEM((line, 8, LANES), jnp.float32),
            pltpu.VMEM((pair, 8, pair * 2 * band_count), jnp.float32),
            pltpu.VMEM((8, LANES), jnp.float32),
            pltpu.VMEM((3, width), jnp.int32),
            dma((3,)),
            dma((2, line, pair, PIECES)),
            dma((line, pair, PIECES)),
            dma((PIECES + 2,)),
            dma((PIECES + 2,)),
            dma((line, peers - 1)),
            dma((line, peers - 1)),
            dma((peers - 1,)),
            dma((peers - 1,)),
            dma((line - 1,)),
            dma((line - 1,)),
        ],
        compiler_params=pltpu.CompilerParams(collective_id=0, has_side_effects=True, vmem_limit_bytes=56 * 2**20),
    )(
        wave_coeffs.reshape(2 * band_count, width),
        projectors.reshape(2 * PROJ, width),
        miller_index,
        lattice,
        occupation.reshape(1, band_count),
        species,
        proj_count,
        coupling,
    )


def solution(mesh):
    return jax.shard_map(
        functools.partial(body, mesh.shape["band"], mesh.shape["gvec"]),
        mesh=mesh,
        in_specs=(
            P(None, "band", "gvec"),
            P(None, "band", "gvec"),
            P(None, "gvec"),
            P(),
            P("band"),
            P(),
            P(),
            P(),
        ),
        out_specs=(P(None, "band"), P()),
        check_vma=False,
    )
```
